32 devices in a mesh: cand: 2 (over y), gx: 8 (over z, x), gy: 2 (over core).
Axes of the slice: x: 2, y: 2, z: 4, core: 2. Of those that a mesh axis runs over, the one named last changes fastest.
Arguments:
- electric: float32 [2, 3, 64, 64, 128], P(None, None, ('cand', 'gx'), 'gy'), parts along dimension 2, may hold values from -6 to 6
- magnetic: float32 [2, 3, 64, 64, 128], P(None, None, ('cand', 'gx'), 'gy'), parts along dimension 2, may hold values from -6 to 6
- density: float32 [64, 64, 128], P(('cand', 'gx'), 'gy'), parts along dimension 0, may hold values from 0 to 0.1
- design_mask: int32 [64, 64, 128], P(('cand', 'gx'), 'gy'), parts along dimension 0, may hold values 0 or 1
- planes: int32 [4], P('cand'), parts along dimension 0, may hold values from 8 to 119
- profiles: float32 [2, 64, 64], P(None, ('cand', 'gx'), 'gy'), parts along dimension 1, may hold values from -6 to 6
- waveforms: float32 [2, 16], P(None, 'cand'), parts along dimension 1, may hold values from -4 to 4
Outputs:
- electric_out: float32 [2, 3, 64, 64, 128], P(None, None, ('cand', 'gx'), 'gy'), parts along dimension 2
- magnetic_out: float32 [2, 3, 64, 64, 128], P(None, None, ('cand', 'gx'), 'gy'), parts along dimension 2
- gradient: float32 [64, 64, 128], P(('cand', 'gx'), 'gy'), parts along dimension 0
The draws below stay inside these ranges and needn't reach their ends.
There are 2 independent parts, one for each index of `cand`. The reference program is written for one: setup_inputs(seed, part) draws one part's arguments, and reference() takes and returns one part's arrays. A program takes and returns all parts, laid end to end along the dimension named above; each array names one. Nothing has to cross between parts.
All inputs are finite; a program needn't handle non-finite values. No bound on the sum of `design_mask` on one device may be relied on, other than what follows from the above.
Results may differ from the reference program's by a relative error of at most 0.00016.
Values sent between devices are 32-bit elements; how exact they have to be, the bound alone decides.
A program may use at most 64 MiB of HBM per device.

```python
import jax
import jax.numpy as jnp
from jax import lax

NZ = 128
STEPS = 8
PMLW = 8
NX = 32
NY = 64


def plant(values, own_key, least, high):
    index_at = [jax.random.randint(jax.random.fold_in(own_key, axis), (), 0, length) for axis, length in enumerate(values.shape)]
    main_axis = values.shape.index(max(values.shape))
    beside = index_at[:main_axis] + [(index_at[main_axis] + 1) % values.shape[main_axis]] + index_at[main_axis + 1:]
    return values.at[tuple(index_at)].set(least).at[tuple(beside)].set(high)


def shard_levels(key, shape, split, smallest, top_value):
    level, own = 1.0, jax.random.fold_in(key, 6)
    for position, blocks in split:
        steps = jnp.exp(jax.random.uniform(jax.random.fold_in(own, position), (blocks,), jnp.float32, smallest / len(split), top_value / len(split)))
        level = level * jnp.repeat(steps, shape[position] // blocks).reshape([-1 if axis == position else 1 for axis in range(len(shape))])
    return level


def normal_values(rng, shape, spread, reach, cuts=(), held_as=jnp.bfloat16):
    entries = spread * jax.random.normal(rng, shape, jnp.float32)
    if cuts:
        entries = entries * shard_levels(rng, shape, cuts, -0.22, 0.18)
    return jnp.clip(entries, -reach, reach).astype(held_as)


def setup_inputs(seed: int = 0, part: int = 0) -> dict:
    splits = jax.random.split(jax.random.key(seed), 8)
    part_splits = jax.random.split(jax.random.fold_in(splits[7], part), 8)
    electric = normal_values(part_splits[0], (2, 3, NX, NY, NZ), 1.0, 6.0, ((2, 8), (3, 2)), jnp.float32)
    magnetic = normal_values(part_splits[1], (2, 3, NX, NY, NZ), 1.0, 6.0, ((2, 8), (3, 2)), jnp.float32)
    density = jnp.clip(0.1 * jax.random.uniform(part_splits[2], (NX, NY, NZ), jnp.float32) ** shard_levels(part_splits[2], (NX, NY, NZ), ((0, 8), (1, 2)), -0.2, 0.2), 0.0, 0.1)
    design_mask = plant((jax.random.randint(part_splits[3], (NX, NY, NZ), 0, 2) < 1).astype(jnp.int32), jax.random.fold_in(part_splits[3], 1), 0, 1)
    planes = jax.random.randint(part_splits[4], (2,), PMLW, NZ - PMLW).astype(jnp.int32)
    profiles = normal_values(part_splits[5], (2, NX, NY), 1.0, 6.0, ((1, 8), (2, 2)), jnp.float32)
    waveforms = normal_values(part_splits[6], (2, STEPS), 1.0, 4.0, (), jnp.float32)
    return dict(electric=electric, magnetic=magnetic, density=density, design_mask=design_mask, planes=planes, profiles=profiles, waveforms=waveforms)


step_dt = 0.7
contrast = 5.0
sigma_max = 2.0
small_eps = 1e-6
inv_spacing = 0.5


def coefficients(depth_cells, layer):
    zpos = jnp.arange(depth_cells).astype(jnp.float32)
    lower = (layer - zpos - 0.5) / layer
    upper = (zpos + 0.5 - (depth_cells - layer)) / layer
    depth = jnp.maximum(jnp.maximum(lower, upper), 0.0)
    sigma = sigma_max * depth * depth * depth
    half = sigma * step_dt / 2.0
    return (1.0 - half) / (1.0 + half), step_dt / (1.0 + half)


def fwd_diff(field, upper, axis):
    rest = lax.slice_in_dim(field, 1, field.shape[axis], axis=axis)
    return jnp.concatenate([rest, upper], axis) - field


def bwd_diff(field, lower, axis):
    rest = lax.slice_in_dim(field, 0, field.shape[axis] - 1, axis=axis)
    return field - jnp.concatenate([lower, rest], axis)


def fwd_z(field):
    return (jnp.concatenate([field[..., 1:], jnp.zeros_like(field[..., :1])], -1) - field) * inv_spacing


def bwd_z(field):
    return (field - jnp.concatenate([jnp.zeros_like(field[..., :1]), field[..., :-1]], -1)) * inv_spacing


def magnetic_update(elec, magn, x_upper, y_upper, decay, gain):
    ex, ey, ez = elec[:, 0], elec[:, 1], elec[:, 2]
    curl_x = fwd_diff(ez, y_upper[:, 1], 2) * inv_spacing - fwd_z(ey)
    curl_y = fwd_z(ex) - fwd_diff(ez, x_upper[:, 1], 1)
    curl_z = fwd_diff(ey, x_upper[:, 0], 1) - fwd_diff(ex, y_upper[:, 0], 2) * inv_spacing
    curl = jnp.stack([curl_x, curl_y, curl_z], 1)
    return decay * magn - gain * curl


def electric_update(elec, magn, x_lower, y_lower, decay, gain, inv_eps, drive):
    hx, hy, hz = magn[:, 0], magn[:, 1], magn[:, 2]
    curl_x = bwd_diff(hz, y_lower[:, 1], 2) * inv_spacing - bwd_z(hy)
    curl_y = bwd_z(hx) - bwd_diff(hz, x_lower[:, 1], 1)
    curl_z = bwd_diff(hy, x_lower[:, 0], 1) - bwd_diff(hx, y_lower[:, 0], 2) * inv_spacing
    new_x = decay * elec[:, 0] + gain * (inv_eps * curl_x - drive)
    new_y = decay * elec[:, 1] + gain * (inv_eps * curl_y)
    new_z = decay * elec[:, 2] + gain * (inv_eps * curl_z)
    return jnp.stack([new_x, new_y, new_z], 1)


def correlate(elec):
    return jnp.sum(elec[0] * elec[1], axis=0)


def reference(electric, magnetic, density, design_mask, planes, profiles, waveforms):
    decay, gain = coefficients(NZ, PMLW)
    flags = design_mask.astype(jnp.float32)
    inv_eps = 1.0 / (1.0 + contrast * density * flags)
    zidx = jnp.arange(NZ).astype(jnp.int32)
    source = profiles[0][:, :, None] * (zidx == planes[0]).astype(jnp.float32)
    adjoint = profiles[1][:, :, None] * (zidx == planes[1]).astype(jnp.float32)
    probe = (zidx == planes[1]).astype(jnp.float32)
    x_zero = jnp.zeros((2, 2, 1, NY, NZ), jnp.float32)
    y_zero = jnp.zeros((2, 2, NX, 1, NZ), jnp.float32)
    elec, magn = electric, magnetic
    corr = jnp.zeros((NX, NY, NZ), jnp.float32)
    for step in range(STEPS):
        magn = magnetic_update(elec, magn, x_zero, y_zero, decay, gain)
        drive = jnp.stack([source * waveforms[0, step], adjoint * waveforms[1, step]])
        elec = electric_update(elec, magn, x_zero, y_zero, decay, gain, inv_eps, drive)
        corr = corr + correlate(elec)
    power = jnp.sum(elec[0] * elec[0] * probe) / (NX * NY)
    gradient = flags * contrast * inv_eps * inv_eps * step_dt * corr / (power + small_eps)
    return elec, magn, gradient
```

```python
import functools

import jax
import jax.numpy as jnp
from jax import lax
from jax.experimental import pallas as pl
from jax.experimental.pallas import tpu as pltpu
from jax.sharding import PartitionSpec as P

STEPS = 8
PMLW = 8
TILE = 8

step_dt = 0.7
contrast = 5.0
sigma_max = 2.0
small_eps = 1e-06
inv_spacing = 0.5

MESH = pl.DeviceIdType.MESH


def coefficients(depth_cells, layer):
    zpos = lax.broadcasted_iota(jnp.int32, (1, depth_cells), 1).astype(jnp.float32)
    lower = (layer - zpos - 0.5) / layer
    upper = (zpos + 0.5 - (depth_cells - layer)) / layer
    depth = jnp.maximum(jnp.maximum(lower, upper), 0.0)
    sigma = sigma_max * depth * depth * depth
    half = sigma * step_dt / 2.0
    return ((1.0 - half) / (1.0 + half), step_dt / (1.0 + half))


def kernel(
    count_x,
    count_y,
    electric,
    magnetic,
    density,
    mask,
    planes,
    profiles,
    waves,
    electric_out,
    magnetic_out,
    gradient_out,
    elec,
    magn,
    scaled,
    source,
    corr,
    front,
    send_up,
    send_down,
    from_low,
    from_high,
    power_mine,
    power_all,
    grad,
    load_sem,
    store_sem,
    side_send,
    side_recv,
    first_send,
    first_recv,
    up_send,
    up_recv,
    down_send,
    down_recv,
    power_send,
    power_recv,
):
    sets, comps, wx, wy, depth_z = electric.shape
    rows = wy + TILE
    last = wx - 1
    gx = lax.axis_index("gx")
    gy = lax.axis_index("gy")
    group = count_x * count_y
    me = gx * count_y + gy
    other = {"gy": 1 - gy}
    upper = {"gx": lax.rem(gx + 1, count_x)}
    lower = {"gx": lax.rem(gx + count_x - 1, count_x)}
    own = pl.multiple_of(gy * TILE, TILE)

    def peer(j):
        at = lax.rem(me + j, group)
        return at, {"gx": at // count_y, "gy": lax.rem(at, count_y)}

    barrier = pltpu.get_barrier_semaphore()

    def greet(j, carry):
        pl.semaphore_signal(barrier, inc=1, device_id=peer(j)[1], device_id_type=MESH)
        return carry

    lax.fori_loop(1, group, greet, 0)

    loads = [
        pltpu.make_async_copy(electric, elec.at[:, :, :, pl.ds(own, wy), :], load_sem.at[0]),
        pltpu.make_async_copy(
            magnetic, magn.at[:, :, pl.ds(1, wx), pl.ds(own + TILE, wy), :], load_sem.at[1]
        ),
    ]
    for load in loads:
        load.start()

    elec[:, :, :, rows:, :] = jnp.zeros((sets, comps, wx, TILE, depth_z), jnp.float32)
    magn[:, :, 1:, :TILE, :] = jnp.zeros((sets, comps, wx, TILE, depth_z), jnp.float32)

    @pl.when(gx == 0)
    def _():
        magn[:, 1:, 0, TILE:, :] = jnp.zeros((sets, comps - 1, rows, depth_z), jnp.float32)

    corr[...] = jnp.zeros_like(corr)
    decay, gain = coefficients(depth_z, PMLW)
    gain_half = gain * inv_spacing
    lane = lax.broadcasted_iota(jnp.int32, (1, depth_z), 1)
    flags = mask[...].astype(jnp.float32)
    inv_eps = 1.0 / (1.0 + contrast * density[...] * flags)
    front[...] = flags * contrast * inv_eps * inv_eps * step_dt
    scaled[:, pl.ds(own, wy), :] = inv_eps * gain
    eye = lax.broadcasted_iota(jnp.int32, (wy, wy), 0) == lax.broadcasted_iota(
        jnp.int32, (wy, wy), 1
    )
    for s in range(sets):
        hot = jnp.where(lane == planes[s], gain, 0.0)
        for x in range(wx):
            row = jnp.broadcast_to(profiles[s, x : x + 1, :], (wy, wy))
            column = jnp.sum(jnp.where(eye, row, 0.0), axis=1, keepdims=True)
            source[s, x, pl.ds(own, wy), :] = column * hot

    for load in loads:
        load.wait()
    pl.semaphore_wait(barrier, group - 1)

    take = pl.multiple_of((1 - gy) * (wy - TILE) + gy * TILE, TILE)
    put = pl.multiple_of(gy * wy, TILE)
    spots = [
        (elec, (slice(None),) * 3, 0),
        (magn, (slice(None), slice(None), pl.ds(1, wx)), TILE),
        (scaled, (slice(None),), 0),
        (source, (slice(None),) * 2, 0),
    ]
    sides = [
        pltpu.make_async_remote_copy(
            src_ref=ref.at[(*lead, pl.ds(take + base, TILE), slice(None))],
            dst_ref=ref.at[(*lead, pl.ds(put + base, TILE), slice(None))],
            send_sem=side_send.at[k],
            recv_sem=side_recv.at[k],
            device_id=other,
            device_id_type=MESH,
        )
        for k, (ref, lead, base) in enumerate(spots)
    ]
    for side in sides:
        side.start()
    for side in sides:
        side.wait()

    def next_z(f):
        return jnp.where(lane < depth_z - 1, pltpu.roll(f, depth_z - 1, 1), 0.0)

    def previous_z(f):
        return jnp.where(lane > 0, pltpu.roll(f, 1, 1), 0.0)

    def up_copy(e, s):
        return pltpu.make_async_remote_copy(
            src_ref=send_up.at[e, s],
            dst_ref=from_low.at[e, s],
            send_sem=up_send.at[e, s],
            recv_sem=up_recv.at[e, s],
            device_id=upper,
            device_id_type=MESH,
        )

    def down_copy(e, s):
        return pltpu.make_async_remote_copy(
            src_ref=send_down.at[e, s],
            dst_ref=from_high.at[e, s],
            send_sem=down_send.at[e, s],
            recv_sem=down_recv.at[e, s],
            device_id=lower,
            device_id_type=MESH,
        )

    def first_copy(s):
        return pltpu.make_async_remote_copy(
            src_ref=magn.at[s, pl.ds(1, 2), wx, pl.ds(TILE, rows), :],
            dst_ref=magn.at[s, pl.ds(1, 2), 0, pl.ds(TILE, rows), :],
            send_sem=first_send.at[s],
            recv_sem=first_recv.at[s],
            device_id=upper,
            device_id_type=MESH,
        )

    def send(e, s):
        ex = elec[s, 0, last, :rows, :]
        send_up[e, s, 0] = (next_z(ex) - ex) * inv_spacing + elec[s, 2, last, :rows, :]
        send_up[e, s, 1] = (elec[s, 0, last, 1 : rows + 1, :] - ex) * inv_spacing + elec[
            s, 1, last, :rows, :
        ]
        send_down[e, s, 0] = elec[s, 1, 0, :rows, :]
        send_down[e, s, 1] = elec[s, 2, 0, :rows, :]

        @pl.when(gx < count_x - 1)
        def _():
            up_copy(e, s).start()

        @pl.when(gx > 0)
        def _():
            down_copy(e, s).start()

    def magnetic_at(s, x, ey_next, ez_next):
        ex = elec[s, 0, x, :rows, :]
        ey = elec[s, 1, x, :rows, :]
        ez = elec[s, 2, x, :rows, :]
        ex_y = elec[s, 0, x, 1 : rows + 1, :]
        ez_y = elec[s, 2, x, 1 : rows + 1, :]
        hx = magn[s, 0, x + 1, TILE:, :]
        hy = magn[s, 1, x + 1, TILE:, :]
        hz = magn[s, 2, x + 1, TILE:, :]
        magn[s, 0, x + 1, TILE:, :] = decay * hx - gain_half * ((ez_y - ez) - (next_z(ey) - ey))
        magn[s, 1, x + 1, TILE:, :] = (
            decay * hy - gain_half * (next_z(ex) - ex) + gain * (ez_next - ez)
        )
        magn[s, 2, x + 1, TILE:, :] = (
            decay * hz - gain * (ey_next - ey) + gain_half * (ex_y - ex)
        )

    def electric_at(t, s, x):
        hx = magn[s, 0, x + 1, TILE:, :]
        hy = magn[s, 1, x + 1, TILE:, :]
        hz = magn[s, 2, x + 1, TILE:, :]
        hx_y = magn[s, 0, x + 1, TILE - 1 : TILE - 1 + rows, :]
        hz_y = magn[s, 2, x + 1, TILE - 1 : TILE - 1 + rows, :]
        hy_x = magn[s, 1, x, TILE:, :]
        hz_x = magn[s, 2, x, TILE:, :]
        weight = scaled[x]
        half = weight * inv_spacing
        elec[s, 0, x, :rows, :] = (
            decay * elec[s, 0, x, :rows, :]
            + half * ((hz - hz_y) - (hy - previous_z(hy)))
            - source[s, x] * waves[s, t]
        )
        elec[s, 1, x, :rows, :] = (
            decay * elec[s, 1, x, :rows, :]
            + half * (hx - previous_z(hx))
            - weight * (hz - hz_x)
        )
        elec[s, 2, x, :rows, :] = (
            decay * elec[s, 2, x, :rows, :] + weight * (hy - hy_x) - half * (hx - hx_y)
        )

    def inner(t, s):
        for x in range(last):
            magnetic_at(s, x, elec[s, 1, x + 1, :rows, :], elec[s, 2, x + 1, :rows, :])
        for x in range(1, last):
            electric_at(t, s, x)

    def outer(t, s):
        @pl.when(gx > 0)
        def _():
            up_copy(t, s).wait_recv()

        @pl.when(gx < count_x - 1)
        def _():
            down_copy(t, s).wait_recv()

        inside = jnp.where(gx < count_x - 1, 1, 0)
        keep = jnp.broadcast_to(inside, (rows, depth_z)) == 1
        magnetic_at(
            s,
            last,
            jnp.where(keep, from_high[t, s, 0], 0.0),
            jnp.where(keep, from_high[t, s, 1], 0.0),
        )
        hy = magn[s, 1, 0, TILE:, :]
        hz = magn[s, 2, 0, TILE:, :]
        there = jnp.broadcast_to(jnp.where(gx > 0, 1, 0), (rows, depth_z)) == 1
        magn[s, 1, 0, TILE:, :] = jnp.where(
            there, decay * hy - gain * (from_low[t, s, 0] - elec[s, 2, 0, :rows, :]), 0.0
        )
        magn[s, 2, 0, TILE:, :] = jnp.where(
            there, decay * hz - gain * (elec[s, 1, 0, :rows, :] - from_low[t, s, 1]), 0.0
        )
        electric_at(t, s, 0)
        if last > 0:
            electric_at(t, s, last)

    def correlate():
        for x in range(wx):
            total = corr[x]
            for c in range(comps):
                total = total + elec[0, c, x, :rows, :] * elec[1, c, x, :rows, :]
            corr[x] = total

    for s in range(sets):
        send(0, s)

        @pl.when(gx < count_x - 1)
        def _():
            first_copy(s).start()

    for s in range(sets):
        inner(0, s)

    for s in range(sets):

        @pl.when(gx > 0)
        def _():
            first_copy(s).wait_recv()

        @pl.when(gx < count_x - 1)
        def _():
            first_copy(s).wait_send()

    def step(t, carry):
        for s in range(sets):
            outer(t, s)
            send(t + 1, s)
        correlate()
        for s in range(sets):
            inner(t + 1, s)
        return carry

    lax.fori_loop(0, STEPS - 1, step, 0)

    def give(s):
        return [
            pltpu.make_async_copy(
                elec.at[s, :, :, pl.ds(own, wy), :], electric_out.at[s], store_sem.at[0, s]
            ),
            pltpu.make_async_copy(
                magn.at[s, :, pl.ds(1, wx), pl.ds(own + TILE, wy), :],
                magnetic_out.at[s],
                store_sem.at[1, s],
            ),
        ]

    def power_copy(j, sender):
        at, device = peer(j)
        return pltpu.make_async_remote_copy(
            src_ref=power_mine,
            dst_ref=power_all.at[sender],
            send_sem=power_send.at[at],
            recv_sem=power_recv.at[sender],
            device_id=device,
            device_id_type=MESH,
        )

    outer(STEPS - 1, 0)
    local = jnp.zeros((TILE, depth_z), jnp.float32)
    for c in range(comps):
        for x in range(wx):
            field = elec[0, c, x, pl.ds(own, wy), :]
            square = field * field
            for k in range(wy // TILE):
                local = local + square[k * TILE : (k + 1) * TILE, :]
    local = jnp.where(lane == planes[1], local, 0.0)
    power_mine[...] = local
    power_all[me] = local

    def share(j, carry):
        power_copy(j, me).start()
        return carry

    lax.fori_loop(1, group, share, 0)
    for copy in give(0):
        copy.start()

    outer(STEPS - 1, 1)
    for copy in give(1):
        copy.start()
    correlate()

    def collect(j, carry):
        at, _ = peer(j)
        power_copy(j, at).wait_recv()
        return carry

    lax.fori_loop(1, group, collect, 0)

    def add(j, total):
        return total + power_all[j]

    total = lax.fori_loop(0, group, add, jnp.zeros((TILE, depth_z), jnp.float32))
    power = jnp.sum(jnp.sum(total, axis=0, keepdims=True), axis=1, keepdims=True)
    power = power / (wx * count_x * wy * count_y)
    scale = 1.0 / (power + small_eps)
    for x in range(wx):
        grad[x] = front[x] * corr[x, pl.ds(own, wy), :] * scale
    last_copy = pltpu.make_async_copy(grad, gradient_out, load_sem.at[0])
    last_copy.start()

    def sent(j, carry):
        power_copy(j, me).wait_send()
        return carry

    lax.fori_loop(1, group, sent, 0)

    def drain(e, carry):
        for s in range(sets):

            @pl.when(gx < count_x - 1)
            def _():
                up_copy(e, s).wait_send()

            @pl.when(gx > 0)
            def _():
                down_copy(e, s).wait_send()

        return carry

    lax.fori_loop(0, STEPS, drain, 0)
    for s in range(sets):
        for copy in give(s):
            copy.wait()
    last_copy.wait()


def shards(count_x, count_y, electric, magnetic, density, design_mask, planes, profiles, waveforms):
    sets, comps, wx, wy, depth_z = electric.shape
    assert count_y == 2 and STEPS <= TILE
    rows = wy + TILE
    group = count_x * count_y
    f32 = jnp.float32
    dma = pltpu.SemaphoreType.DMA
    hbm = pl.BlockSpec(memory_space=pl.ANY)
    vmem = pl.BlockSpec(memory_space=pltpu.VMEM)
    smem = pl.BlockSpec(memory_space=pltpu.SMEM)
    return pl.pallas_call(
        functools.partial(kernel, count_x, count_y),
        out_shape=(
            jax.ShapeDtypeStruct(electric.shape, f32),
            jax.ShapeDtypeStruct(magnetic.shape, f32),
            jax.ShapeDtypeStruct(density.shape, f32),
        ),
        in_specs=[hbm, hbm, vmem, vmem, smem, vmem, smem],
        out_specs=(hbm, hbm, hbm),
        scratch_shapes=[
            pltpu.VMEM((sets, comps, wx, rows + TILE, depth_z), f32),
            pltpu.VMEM((sets, comps, wx + 1, rows + TILE, depth_z), f32),
            pltpu.VMEM((wx, rows, depth_z), f32),
            pltpu.VMEM((sets, wx, rows, depth_z), f32),
            pltpu.VMEM((wx, rows, depth_z), f32),
            pltpu.VMEM((wx, wy, depth_z), f32),
            pltpu.VMEM((STEPS, sets, 2, rows, depth_z), f32),
            pltpu.VMEM((STEPS, sets, 2, rows, depth_z), f32),
            pltpu.VMEM((STEPS, sets, 2, rows, depth_z), f32),
            pltpu.VMEM((STEPS, sets, 2, rows, depth_z), f32),
            pltpu.VMEM((TILE, depth_z), f32),
            pltpu.VMEM((group, TILE, depth_z), f32),
            pltpu.VMEM((wx, wy, depth_z), f32),
            dma((2,)),
            dma((2, sets)),
            dma((4,)),
            dma((4,)),
            dma((sets,)),
            dma((sets,)),
            dma((STEPS, sets)),
            dma((STEPS, sets)),
            dma((STEPS, sets)),
            dma((STEPS, sets)),
            dma((group,)),
            dma((group,)),
        ],
        compiler_params=pltpu.CompilerParams(collective_id=0, has_side_effects=True),
    )(electric, magnetic, density, design_mask, planes, profiles, waveforms)


def solution(mesh):
    return jax.shard_map(
        functools.partial(shards, mesh.shape["gx"], mesh.shape["gy"]),
        mesh=mesh,
        in_specs=(
            P(None, None, ("cand", "gx"), "gy", None),
            P(None, None, ("cand", "gx"), "gy", None),
            P(("cand", "gx"), "gy", None),
            P(("cand", "gx"), "gy", None),
            P("cand"),
            P(None, ("cand", "gx"), "gy"),
            P(None, "cand"),
        ),
        out_specs=(
            P(None, None, ("cand", "gx"), "gy", None),
            P(None, None, ("cand", "gx"), "gy", None),
            P(("cand", "gx"), "gy", None),
        ),
        check_vma=False,
    )
```

```python
import functools

import jax
import jax.numpy as jnp
from jax import lax
from jax.experimental import pallas as pl
from jax.experimental.pallas import tpu as pltpu
from jax.sharding import PartitionSpec as P

STEPS = 8
PMLW = 8
TILE = 8

step_dt = 0.7
contrast = 5.0
sigma_max = 2.0
small_eps = 1e-06
inv_spacing = 0.5

MESH = pl.DeviceIdType.MESH


def coefficients(depth_cells, layer):
    zpos = lax.broadcasted_iota(jnp.int32, (1, depth_cells), 1).astype(jnp.float32)
    lower = (layer - zpos - 0.5) / layer
    upper = (zpos + 0.5 - (depth_cells - layer)) / layer
    depth = jnp.maximum(jnp.maximum(lower, upper), 0.0)
    sigma = sigma_max * depth * depth * depth
    half = sigma * step_dt / 2.0
    return ((1.0 - half) / (1.0 + half), step_dt / (1.0 + half))


def kernel(
    count_x,
    count_y,
    electric,
    magnetic,
    density_far,
    mask_far,
    planes_far,
    profiles_far,
    waves_far,
    electric_out,
    magnetic_out,
    gradient_out,
    elec,
    magn,
    scaled,
    source,
    corr,
    front,
    send_up,
    send_down,
    from_low,
    from_high,
    power_mine,
    power_all,
    grad,
    density,
    mask,
    planes,
    profiles,
    waves,
    load_sem,
    store_sem,
    side_send,
    side_recv,
    up_send,
    up_recv,
    down_send,
    down_recv,
    power_send,
    power_recv,
):
    sets, comps, wx, wy, depth_z = electric.shape
    rows = wy + TILE
    last = wx - 1
    gx = lax.axis_index("gx")
    gy = lax.axis_index("gy")
    group = count_x * count_y
    me = gx * count_y + gy
    other = {"gy": 1 - gy}
    upper = {"gx": lax.rem(gx + 1, count_x)}
    lower = {"gx": lax.rem(gx + count_x - 1, count_x)}
    own = pl.multiple_of(gy * TILE, TILE)

    def peer(j):
        at = lax.rem(me + j, group)
        return at, {"gx": at // count_y, "gy": lax.rem(at, count_y)}


    small = [
        pltpu.make_async_copy(far, near, load_sem.at[2 + k])
        for k, (far, near) in enumerate(
            (
                (density_far, density),
                (mask_far, mask),
                (profiles_far, profiles),
                (planes_far, planes),
                (waves_far, waves),
            )
        )
    ]
    loads = [
        pltpu.make_async_copy(electric, elec.at[:, :, :, pl.ds(own, wy), :], load_sem.at[0]),
        pltpu.make_async_copy(
            magnetic, magn.at[:, :, pl.ds(1, wx), pl.ds(own + TILE, wy), :], load_sem.at[1]
        ),
    ]
    for load in small + loads:
        load.start()

    elec[:, :, :, rows:, :] = jnp.zeros((sets, comps, wx, TILE, depth_z), jnp.float32)
    magn[:, :, 1:, :TILE, :] = jnp.zeros((sets, comps, wx, TILE, depth_z), jnp.float32)

    barrier = pltpu.get_barrier_semaphore()

    def greet(j, carry):
        pl.semaphore_signal(barrier, inc=1, device_id=peer(j)[1], device_id_type=MESH)
        return carry

    lax.fori_loop(1, group, greet, 0)

    corr[...] = jnp.zeros_like(corr)
    decay, gain = coefficients(depth_z, PMLW)
    gain_half = gain * inv_spacing
    lane = lax.broadcasted_iota(jnp.int32, (1, depth_z), 1)
    for load in small:
        load.wait()
    flags = mask[...].astype(jnp.float32)
    inv_eps = 1.0 / (1.0 + contrast * density[...] * flags)
    front[...] = flags * contrast * inv_eps * inv_eps * step_dt
    scaled[:, pl.ds(own, wy), :] = inv_eps * gain
    eye = lax.broadcasted_iota(jnp.int32, (wy, wy), 0) == lax.broadcasted_iota(
        jnp.int32, (wy, wy), 1
    )
    for s in range(sets):
        hot = jnp.where(lane == planes[s], gain, 0.0)
        for x in range(wx):
            row = jnp.broadcast_to(profiles[s, x : x + 1, :], (wy, wy))
            column = jnp.sum(jnp.where(eye, row, 0.0), axis=1, keepdims=True)
            source[s, x, pl.ds(own, wy), :] = column * hot

    for load in loads:
        load.wait()
    pl.semaphore_wait(barrier, group - 1)

    take = pl.multiple_of((1 - gy) * (wy - TILE) + gy * TILE, TILE)
    put = pl.multiple_of(gy * wy, TILE)
    spots = [
        (elec, (slice(None),) * 3, 0),
        (magn, (slice(None), slice(None), pl.ds(1, wx)), TILE),
        (scaled, (slice(None),), 0),
        (source, (slice(None),) * 2, 0),
    ]
    sides = [
        pltpu.make_async_remote_copy(
            src_ref=ref.at[(*lead, pl.ds(take + base, TILE), slice(None))],
            dst_ref=ref.at[(*lead, pl.ds(put + base, TILE), slice(None))],
            send_sem=side_send.at[k],
            recv_sem=side_recv.at[k],
            device_id=other,
            device_id_type=MESH,
        )
        for k, (ref, lead, base) in enumerate(spots)
    ]
    for side in sides:
        side.start()
    for side in sides:
        side.wait()

    def next_z(f):
        return jnp.where(lane < depth_z - 1, pltpu.roll(f, depth_z - 1, 1), 0.0)

    def previous_z(f):
        return jnp.where(lane > 0, pltpu.roll(f, 1, 1), 0.0)

    def up_copy(e, s):
        return pltpu.make_async_remote_copy(
            src_ref=send_up.at[e, s],
            dst_ref=from_low.at[e, s],
            send_sem=up_send.at[e, s],
            recv_sem=up_recv.at[e, s],
            device_id=upper,
            device_id_type=MESH,
        )

    def down_copy(e, s):
        return pltpu.make_async_remote_copy(
            src_ref=send_down.at[e, s],
            dst_ref=from_high.at[e, s],
            send_sem=down_send.at[e, s],
            recv_sem=down_recv.at[e, s],
            device_id=lower,
            device_id_type=MESH,
        )

    def send_high(e, s):
        ex = elec[s, 0, last, :rows, :]
        ey = elec[s, 1, last, :rows, :]
        ez = elec[s, 2, last, :rows, :]
        ex_y = elec[s, 0, last, 1 : rows + 1, :]
        hy = magn[s, 1, wx, TILE:, :]
        hz = magn[s, 2, wx, TILE:, :]
        send_up[e, s, 0] = decay * hy - gain_half * (next_z(ex) - ex) - gain * ez
        send_up[e, s, 1] = decay * hz + gain * ey + gain_half * (ex_y - ex)

        @pl.when(gx < count_x - 1)
        def _():
            up_copy(e, s).start()

    def send_low(e, s):
        send_down[e, s, 0] = elec[s, 1, 0, :rows, :]
        send_down[e, s, 1] = elec[s, 2, 0, :rows, :]

        @pl.when(gx > 0)
        def _():
            down_copy(e, s).start()

    def magnetic_at(s, x, ey_next, ez_next):
        ex = elec[s, 0, x, :rows, :]
        ey = elec[s, 1, x, :rows, :]
        ez = elec[s, 2, x, :rows, :]
        ex_y = elec[s, 0, x, 1 : rows + 1, :]
        ez_y = elec[s, 2, x, 1 : rows + 1, :]
        hx = magn[s, 0, x + 1, TILE:, :]
        hy = magn[s, 1, x + 1, TILE:, :]
        hz = magn[s, 2, x + 1, TILE:, :]
        magn[s, 0, x + 1, TILE:, :] = decay * hx - gain_half * ((ez_y - ez) - (next_z(ey) - ey))
        magn[s, 1, x + 1, TILE:, :] = (
            decay * hy - gain_half * (next_z(ex) - ex) + gain * (ez_next - ez)
        )
        magn[s, 2, x + 1, TILE:, :] = (
            decay * hz - gain * (ey_next - ey) + gain_half * (ex_y - ex)
        )

    def electric_at(t, s, x):
        hx = magn[s, 0, x + 1, TILE:, :]
        hy = magn[s, 1, x + 1, TILE:, :]
        hz = magn[s, 2, x + 1, TILE:, :]
        hx_y = magn[s, 0, x + 1, TILE - 1 : TILE - 1 + rows, :]
        hz_y = magn[s, 2, x + 1, TILE - 1 : TILE - 1 + rows, :]
        hy_x = magn[s, 1, x, TILE:, :]
        hz_x = magn[s, 2, x, TILE:, :]
        weight = scaled[x]
        half = weight * inv_spacing
        elec[s, 0, x, :rows, :] = (
            decay * elec[s, 0, x, :rows, :]
            + half * ((hz - hz_y) - (hy - previous_z(hy)))
            - source[s, x] * waves[s, t]
        )
        elec[s, 1, x, :rows, :] = (
            decay * elec[s, 1, x, :rows, :]
            + half * (hx - previous_z(hx))
            - weight * (hz - hz_x)
        )
        elec[s, 2, x, :rows, :] = (
            decay * elec[s, 2, x, :rows, :] + weight * (hy - hy_x) - half * (hx - hx_y)
        )

    def inner(t, s):
        for x in range(last):
            magnetic_at(s, x, elec[s, 1, x + 1, :rows, :], elec[s, 2, x + 1, :rows, :])
        for x in range(1, last):
            electric_at(t, s, x)

    def outer_high(t, s):
        @pl.when(gx < count_x - 1)
        def _():
            down_copy(t, s).wait_recv()

        keep = jnp.broadcast_to(jnp.where(gx < count_x - 1, 1, 0), (rows, depth_z)) == 1
        magnetic_at(
            s,
            last,
            jnp.where(keep, from_high[t, s, 0], 0.0),
            jnp.where(keep, from_high[t, s, 1], 0.0),
        )
        electric_at(t, s, last)

    def outer_low(t, s):
        @pl.when(gx > 0)
        def _():
            up_copy(t, s).wait_recv()

        keep = jnp.broadcast_to(jnp.where(gx > 0, 1, 0), (rows, depth_z)) == 1
        magn[s, 1, 0, TILE:, :] = jnp.where(
            keep, from_low[t, s, 0] + gain * elec[s, 2, 0, :rows, :], 0.0
        )
        magn[s, 2, 0, TILE:, :] = jnp.where(
            keep, from_low[t, s, 1] - gain * elec[s, 1, 0, :rows, :], 0.0
        )
        electric_at(t, s, 0)

    def edges(t, order, more):
        for kind, s in order:
            if kind:
                outer_high(t, s)
                if more:
                    send_high(t + 1, s)
            else:
                outer_low(t, s)
                if more:
                    send_low(t + 1, s)

    even = lax.rem(gx, 2) == 0

    def correlate():
        for x in range(wx):
            total = corr[x]
            for c in range(comps):
                total = total + elec[0, c, x, :rows, :] * elec[1, c, x, :rows, :]
            corr[x] = total

    for s in range(sets):
        send_high(0, s)
        send_low(0, s)

    for s in range(sets):
        inner(0, s)

    def step(t, carry):
        for parity in range(2):

            @pl.when(even if parity == 0 else jnp.logical_not(even))
            def _():
                near = 1 - parity
                edges(t, ((1 - near, 0), (near, 0), (1 - near, 1), (near, 1)), True)

        correlate()
        for s in range(sets):
            inner(t + 1, s)
        return carry

    lax.fori_loop(0, STEPS - 1, step, 0)

    def give(s):
        return [
            pltpu.make_async_copy(
                elec.at[s, :, :, pl.ds(own, wy), :], electric_out.at[s], store_sem.at[0, s]
            ),
            pltpu.make_async_copy(
                magn.at[s, :, pl.ds(1, wx), pl.ds(own + TILE, wy), :],
                magnetic_out.at[s],
                store_sem.at[1, s],
            ),
        ]

    def power_copy(j, sender):
        at, device = peer(j)
        return pltpu.make_async_remote_copy(
            src_ref=power_mine,
            dst_ref=power_all.at[sender],
            send_sem=power_send.at[at],
            recv_sem=power_recv.at[sender],
            device_id=device,
            device_id_type=MESH,
        )

    outer_low(STEPS - 1, 0)
    outer_high(STEPS - 1, 0)
    local = jnp.zeros((TILE, depth_z), jnp.float32)
    for c in range(comps):
        for x in range(wx):
            field = elec[0, c, x, pl.ds(own, wy), :]
            square = field * field
            for k in range(wy // TILE):
                local = local + square[k * TILE : (k + 1) * TILE, :]
    local = jnp.where(lane == planes[1], jnp.sum(local, axis=0, keepdims=True), 0.0)
    power_mine[...] = local
    power_all[me] = local

    def share(j, carry):
        power_copy(j, me).start()
        return carry

    lax.fori_loop(1, group, share, 0)
    for copy in give(0):
        copy.start()

    outer_low(STEPS - 1, 1)
    outer_high(STEPS - 1, 1)
    for copy in give(1):
        copy.start()
    correlate()

    def collect(j, carry):
        at, _ = peer(j)
        power_copy(j, at).wait_recv()
        return carry

    lax.fori_loop(1, group, collect, 0)

    def add(j, total):
        return total + power_all[j]

    total = lax.fori_loop(0, group, add, jnp.zeros((1, depth_z), jnp.float32))
    power = jnp.sum(total, axis=1, keepdims=True)
    power = power / (wx * count_x * wy * count_y)
    scale = 1.0 / (power + small_eps)
    for x in range(wx):
        grad[x] = front[x] * corr[x, pl.ds(own, wy), :] * scale
    last_copy = pltpu.make_async_copy(grad, gradient_out, load_sem.at[0])
    last_copy.start()

    def sent(j, carry):
        power_copy(j, me).wait_send()
        return carry

    lax.fori_loop(1, group, sent, 0)

    def drain(e, carry):
        for s in range(sets):

            @pl.when(gx < count_x - 1)
            def _():
                up_copy(e, s).wait_send()

            @pl.when(gx > 0)
            def _():
                down_copy(e, s).wait_send()

        return carry

    lax.fori_loop(0, STEPS, drain, 0)
    for s in range(sets):
        for copy in give(s):
            copy.wait()
    last_copy.wait()


def shards(count_x, count_y, electric, magnetic, density, design_mask, planes, profiles, waveforms):
    sets, comps, wx, wy, depth_z = electric.shape
    assert count_y == 2 and STEPS <= TILE and wx > 1
    rows = wy + TILE
    group = count_x * count_y
    f32 = jnp.float32
    dma = pltpu.SemaphoreType.DMA
    hbm = pl.BlockSpec(memory_space=pl.ANY)
    return pl.pallas_call(
        functools.partial(kernel, count_x, count_y),
        out_shape=(
            jax.ShapeDtypeStruct(electric.shape, f32),
            jax.ShapeDtypeStruct(magnetic.shape, f32),
            jax.ShapeDtypeStruct(density.shape, f32),
        ),
        in_specs=[hbm] * 7,
        out_specs=(hbm, hbm, hbm),
        scratch_shapes=[
            pltpu.VMEM((sets, comps, wx, rows + TILE, depth_z), f32),
            pltpu.VMEM((sets, comps, wx + 1, rows + TILE, depth_z), f32),
            pltpu.VMEM((wx, rows, depth_z), f32),
            pltpu.VMEM((sets, wx, rows, depth_z), f32),
            pltpu.VMEM((wx, rows, depth_z), f32),
            pltpu.VMEM((wx, wy, depth_z), f32),
            pltpu.VMEM((STEPS, sets, 2, rows, depth_z), f32),
            pltpu.VMEM((STEPS, sets, 2, rows, depth_z), f32),
            pltpu.VMEM((STEPS, sets, 2, rows, depth_z), f32),
            pltpu.VMEM((STEPS, sets, 2, rows, depth_z), f32),
            pltpu.VMEM((1, depth_z), f32),
            pltpu.VMEM((group, 1, depth_z), f32),
            pltpu.VMEM((wx, wy, depth_z), f32),
            pltpu.VMEM(density.shape, f32),
            pltpu.VMEM(density.shape, jnp.int32),
            pltpu.SMEM(planes.shape, jnp.int32),
            pltpu.VMEM(profiles.shape, f32),
            pltpu.SMEM(waveforms.shape, f32),
            dma((7,)),
            dma((2, sets)),
            dma((4,)),
            dma((4,)),
            dma((STEPS, sets)),
            dma((STEPS, sets)),
            dma((STEPS, sets)),
            dma((STEPS, sets)),
            dma((group,)),
            dma((group,)),
        ],
        compiler_params=pltpu.CompilerParams(collective_id=0, has_side_effects=True),
    )(electric, magnetic, density, design_mask, planes, profiles, waveforms)


def solution(mesh):
    return jax.shard_map(
        functools.partial(shards, mesh.shape["gx"], mesh.shape["gy"]),
        mesh=mesh,
        in_specs=(
            P(None, None, ("cand", "gx"), "gy", None),
            P(None, None, ("cand", "gx"), "gy", None),
            P(("cand", "gx"), "gy", None),
            P(("cand", "gx"), "gy", None),
            P("cand"),
            P(None, ("cand", "gx"), "gy"),
            P(None, "cand"),
        ),
        out_specs=(
            P(None, None, ("cand", "gx"), "gy", None),
            P(None, None, ("cand", "gx"), "gy", None),
            P(("cand", "gx"), "gy", None),
        ),
        check_vma=False,
    )
```

```python
import functools

import jax
import jax.numpy as jnp
from jax import lax
from jax.experimental import pallas as pl
from jax.experimental.pallas import tpu as pltpu
from jax.sharding import PartitionSpec as P

STEPS = 8
PMLW = 8
TILE = 8

step_dt = 0.7
contrast = 5.0
sigma_max = 2.0
small_eps = 1e-06
inv_spacing = 0.5

MESH = pl.DeviceIdType.MESH


def coefficients(depth_cells, layer):
    zpos = lax.broadcasted_iota(jnp.int32, (1, depth_cells), 1).astype(jnp.float32)
    lower = (layer - zpos - 0.5) / layer
    upper = (zpos + 0.5 - (depth_cells - layer)) / layer
    depth = jnp.maximum(jnp.maximum(lower, upper), 0.0)
    sigma = sigma_max * depth * depth * depth
    half = sigma * step_dt / 2.0
    return ((1.0 - half) / (1.0 + half), step_dt / (1.0 + half))


def kernel(
    count_x,
    count_y,
    electric,
    magnetic,
    density_far,
    mask_far,
    planes_far,
    profiles_far,
    waves_far,
    electric_out,
    magnetic_out,
    gradient_out,
    elec,
    magn,
    scaled,
    source,
    corr,
    front,
    send_up,
    send_down,
    from_low,
    from_high,
    send_side,
    from_side,
    send_slant,
    from_slant,
    power_mine,
    power_all,
    grad,
    density,
    mask,
    planes,
    profiles,
    waves,
    load_sem,
    store_sem,
    side_sent,
    side_recv,
    slant_sent,
    slant_recv,
    up_send,
    up_recv,
    down_send,
    down_recv,
    power_send,
    power_recv,
):
    sets, comps, wx, wy, depth_z = electric.shape
    rows = wy
    edge = wy - 1
    last = wx - 1
    gx = lax.axis_index("gx")
    gy = lax.axis_index("gy")
    group = count_x * count_y
    me = gx * count_y + gy
    other = {"gy": 1 - gy}
    upper = {"gx": lax.rem(gx + 1, count_x)}
    lower = {"gx": lax.rem(gx + count_x - 1, count_x)}
    own = 0

    def peer(j):
        at = lax.rem(me + j, group)
        return at, {"gx": at // count_y, "gy": lax.rem(at, count_y)}


    small = [
        pltpu.make_async_copy(far, near, load_sem.at[2 + k])
        for k, (far, near) in enumerate(
            (
                (density_far, density),
                (mask_far, mask),
                (profiles_far, profiles),
                (planes_far, planes),
                (waves_far, waves),
            )
        )
    ]
    loads = [
        pltpu.make_async_copy(electric, elec.at[:, :, :, pl.ds(own, wy), :], load_sem.at[0]),
        pltpu.make_async_copy(
            magnetic, magn.at[:, :, pl.ds(1, wx), pl.ds(own + TILE, wy), :], load_sem.at[1]
        ),
    ]
    for load in small + loads:
        load.start()

    elec[:, :, :, rows:, :] = jnp.zeros((sets, comps, wx, TILE, depth_z), jnp.float32)
    magn[:, :, 1:, :TILE, :] = jnp.zeros((sets, comps, wx, TILE, depth_z), jnp.float32)

    barrier = pltpu.get_barrier_semaphore()

    def greet(j, carry):
        pl.semaphore_signal(barrier, inc=1, device_id=peer(j)[1], device_id_type=MESH)
        return carry

    lax.fori_loop(1, group, greet, 0)

    corr[...] = jnp.zeros_like(corr)
    decay, gain = coefficients(depth_z, PMLW)
    gain_half = gain * inv_spacing
    lane = lax.broadcasted_iota(jnp.int32, (1, depth_z), 1)
    for load in small:
        load.wait()
    flags = mask[...].astype(jnp.float32)
    inv_eps = 1.0 / (1.0 + contrast * density[...] * flags)
    front[...] = flags * contrast * inv_eps * inv_eps * step_dt
    scaled[:, pl.ds(own, wy), :] = inv_eps * gain
    eye = lax.broadcasted_iota(jnp.int32, (wy, wy), 0) == lax.broadcasted_iota(
        jnp.int32, (wy, wy), 1
    )
    for s in range(sets):
        hot = jnp.where(lane == planes[s], gain, 0.0)
        for x in range(wx):
            row = jnp.broadcast_to(profiles[s, x : x + 1, :], (wy, wy))
            column = jnp.sum(jnp.where(eye, row, 0.0), axis=1, keepdims=True)
            source[s, x, pl.ds(own, wy), :] = column * hot

    for load in loads:
        load.wait()
    pl.semaphore_wait(barrier, group - 1)

    def next_z(f):
        return jnp.where(lane < depth_z - 1, pltpu.roll(f, depth_z - 1, 1), 0.0)

    def previous_z(f):
        return jnp.where(lane > 0, pltpu.roll(f, 1, 1), 0.0)

    def side_copy(e, s):
        return pltpu.make_async_remote_copy(
            src_ref=send_side.at[e, s],
            dst_ref=from_side.at[e, s],
            send_sem=side_sent.at[e, s],
            recv_sem=side_recv.at[e, s],
            device_id=other,
            device_id_type=MESH,
        )

    def slant_copy(e, s):
        return pltpu.make_async_remote_copy(
            src_ref=send_slant.at[e, s],
            dst_ref=from_slant.at[e, s],
            send_sem=slant_sent.at[e, s],
            recv_sem=slant_recv.at[e, s],
            device_id={
                "gx": lax.rem(gx + count_x - 1 + 2 * gy, count_x),
                "gy": 1 - gy,
            },
            device_id_type=MESH,
        )

    def send_beside(e, s):
        @pl.when(gy == 0)
        def _():
            for x in range(wx):
                ex = elec[s, 0, x, edge : edge + 1, :]
                ey = elec[s, 1, x, edge : edge + 1, :]
                ez = elec[s, 2, x, edge : edge + 1, :]
                hx = magn[s, 0, x + 1, TILE + edge : TILE + wy, :]
                hz = magn[s, 2, x + 1, TILE + edge : TILE + wy, :]
                slope = ey if x == last else ey - elec[s, 1, x + 1, edge : edge + 1, :]
                send_side[e, s, x : x + 1, :] = decay * hx + gain_half * (ez + (next_z(ey) - ey))
                send_side[e, s, wx + x : wx + x + 1, :] = (
                    decay * hz + gain * slope - gain_half * ex
                )

        @pl.when(gy == 1)
        def _():
            for x in range(wx):
                send_side[e, s, x : x + 1, :] = elec[s, 0, x, 0:1, :]
                send_side[e, s, wx + x : wx + x + 1, :] = elec[s, 2, x, 0:1, :]

        side_copy(e, s).start()

    def take_beside(t, s):
        side_copy(t, s).wait_recv()

        @pl.when(gy == 0)
        def _():
            for x in range(wx):
                elec[s, 0, x, wy : wy + 1, :] = from_side[t, s, x : x + 1, :]
                elec[s, 2, x, wy : wy + 1, :] = from_side[t, s, wx + x : wx + x + 1, :]

        @pl.when(gy == 1)
        def _():
            for x in range(wx):
                magn[s, 0, x + 1, TILE - 1 : TILE, :] = (
                    from_side[t, s, x : x + 1, :] - gain_half * elec[s, 2, x, 0:1, :]
                )
                magn[s, 2, x + 1, TILE - 1 : TILE, :] = (
                    from_side[t, s, wx + x : wx + x + 1, :] + gain_half * elec[s, 0, x, 0:1, :]
                )

    below_edge = lax.broadcasted_iota(jnp.int32, (rows, depth_z), 0) < edge

    def up_copy(e, s):
        return pltpu.make_async_remote_copy(
            src_ref=send_up.at[e, s],
            dst_ref=from_low.at[e, s],
            send_sem=up_send.at[e, s],
            recv_sem=up_recv.at[e, s],
            device_id=upper,
            device_id_type=MESH,
        )

    def down_copy(e, s):
        return pltpu.make_async_remote_copy(
            src_ref=send_down.at[e, s],
            dst_ref=from_high.at[e, s],
            send_sem=down_send.at[e, s],
            recv_sem=down_recv.at[e, s],
            device_id=lower,
            device_id_type=MESH,
        )

    def send_high(e, s):
        ex = elec[s, 0, last, :rows, :]
        ey = elec[s, 1, last, :rows, :]
        ez = elec[s, 2, last, :rows, :]
        ex_y = jnp.where(below_edge, elec[s, 0, last, 1 : rows + 1, :], 0.0)
        hy = magn[s, 1, wx, TILE:, :]
        hz = magn[s, 2, wx, TILE:, :]
        send_up[e, s, 0] = decay * hy - gain_half * (next_z(ex) - ex) - gain * ez
        send_up[e, s, 1] = decay * hz + gain * ey + gain_half * (ex_y - ex)

        @pl.when(gx < count_x - 1)
        def _():
            up_copy(e, s).start()

        @pl.when((gx < count_x - 1) & (gy == 1))
        def _():
            send_slant[e, s] = elec[s, 0, last, 0:1, :]
            slant_copy(e, s).start()

    def send_low(e, s):
        send_down[e, s, 0] = elec[s, 1, 0, :rows, :]
        send_down[e, s, 1] = elec[s, 2, 0, :rows, :]

        @pl.when(gx > 0)
        def _():
            down_copy(e, s).start()

        @pl.when((gx > 0) & (gy == 0))
        def _():
            send_slant[e, s] = elec[s, 1, 0, edge : edge + 1, :]
            slant_copy(e, s).start()

    def magnetic_at(s, x, ey_next, ez_next):
        ex = elec[s, 0, x, :rows, :]
        ey = elec[s, 1, x, :rows, :]
        ez = elec[s, 2, x, :rows, :]
        ex_y = elec[s, 0, x, 1 : rows + 1, :]
        ez_y = elec[s, 2, x, 1 : rows + 1, :]
        hx = magn[s, 0, x + 1, TILE:, :]
        hy = magn[s, 1, x + 1, TILE:, :]
        hz = magn[s, 2, x + 1, TILE:, :]
        magn[s, 0, x + 1, TILE:, :] = decay * hx - gain_half * ((ez_y - ez) - (next_z(ey) - ey))
        magn[s, 1, x + 1, TILE:, :] = (
            decay * hy - gain_half * (next_z(ex) - ex) + gain * (ez_next - ez)
        )
        magn[s, 2, x + 1, TILE:, :] = (
            decay * hz - gain * (ey_next - ey) + gain_half * (ex_y - ex)
        )

    def electric_at(t, s, x):
        hx = magn[s, 0, x + 1, TILE:, :]
        hy = magn[s, 1, x + 1, TILE:, :]
        hz = magn[s, 2, x + 1, TILE:, :]
        hx_y = magn[s, 0, x + 1, TILE - 1 : TILE - 1 + rows, :]
        hz_y = magn[s, 2, x + 1, TILE - 1 : TILE - 1 + rows, :]
        hy_x = magn[s, 1, x, TILE:, :]
        hz_x = magn[s, 2, x, TILE:, :]
        weight = scaled[x]
        half = weight * inv_spacing
        elec[s, 0, x, :rows, :] = (
            decay * elec[s, 0, x, :rows, :]
            + half * ((hz - hz_y) - (hy - previous_z(hy)))
            - source[s, x] * waves[s, t]
        )
        elec[s, 1, x, :rows, :] = (
            decay * elec[s, 1, x, :rows, :]
            + half * (hx - previous_z(hx))
            - weight * (hz - hz_x)
        )
        elec[s, 2, x, :rows, :] = (
            decay * elec[s, 2, x, :rows, :] + weight * (hy - hy_x) - half * (hx - hx_y)
        )

    def inner(t, s):
        take_beside(t, s)
        for x in range(last):
            magnetic_at(s, x, elec[s, 1, x + 1, :rows, :], elec[s, 2, x + 1, :rows, :])
        for x in range(1, last):
            electric_at(t, s, x)

    def outer_high(t, s):
        @pl.when(gx < count_x - 1)
        def _():
            down_copy(t, s).wait_recv()

        keep = jnp.broadcast_to(jnp.where(gx < count_x - 1, 1, 0), (rows, depth_z)) == 1
        magnetic_at(
            s,
            last,
            jnp.where(keep, from_high[t, s, 0], 0.0),
            jnp.where(keep, from_high[t, s, 1], 0.0),
        )

        @pl.when((gx < count_x - 1) & (gy == 1))
        def _():
            slant_copy(t, s).wait_recv()
            magn[s, 2, wx, TILE - 1 : TILE, :] = (
                magn[s, 2, wx, TILE - 1 : TILE, :] - gain * from_slant[t, s]
            )

        electric_at(t, s, last)

    def outer_low(t, s):
        @pl.when(gx > 0)
        def _():
            up_copy(t, s).wait_recv()

        keep = jnp.broadcast_to(jnp.where(gx > 0, 1, 0), (rows, depth_z)) == 1
        magn[s, 1, 0, TILE:, :] = jnp.where(
            keep, from_low[t, s, 0] + gain * elec[s, 2, 0, :rows, :], 0.0
        )
        magn[s, 2, 0, TILE:, :] = jnp.where(
            keep, from_low[t, s, 1] - gain * elec[s, 1, 0, :rows, :], 0.0
        )

        @pl.when((gx > 0) & (gy == 0))
        def _():
            slant_copy(t, s).wait_recv()
            magn[s, 2, 0, TILE + edge :, :] = (
                magn[s, 2, 0, TILE + edge :, :] + gain_half * from_slant[t, s]
            )

        electric_at(t, s, 0)

    def edges(t, order, more):
        for at, (kind, s) in enumerate(order):
            if kind:
                outer_high(t, s)
                if more:
                    send_high(t + 1, s)
            else:
                outer_low(t, s)
                if more:
                    send_low(t + 1, s)
            if more and at % 2 == 1:
                send_beside(t + 1, s)

    even = lax.rem(gx, 2) == 0

    def correlate():
        for x in range(wx):
            total = corr[x]
            for c in range(comps):
                total = total + elec[0, c, x, :rows, :] * elec[1, c, x, :rows, :]
            corr[x] = total

    for s in range(sets):
        send_high(0, s)
        send_low(0, s)
        send_beside(0, s)

    for s in range(sets):
        inner(0, s)

    def step(t, carry):
        for parity in range(2):

            @pl.when(even if parity == 0 else jnp.logical_not(even))
            def _():
                near = 1 - parity
                edges(t, ((1 - near, 0), (near, 0), (1 - near, 1), (near, 1)), True)

        correlate()
        for s in range(sets):
            inner(t + 1, s)
        return carry

    lax.fori_loop(0, STEPS - 1, step, 0)

    def give(s):
        return [
            pltpu.make_async_copy(
                elec.at[s, :, :, pl.ds(own, wy), :], electric_out.at[s], store_sem.at[0, s]
            ),
            pltpu.make_async_copy(
                magn.at[s, :, pl.ds(1, wx), pl.ds(own + TILE, wy), :],
                magnetic_out.at[s],
                store_sem.at[1, s],
            ),
        ]

    def power_copy(j, sender):
        at, device = peer(j)
        return pltpu.make_async_remote_copy(
            src_ref=power_mine,
            dst_ref=power_all.at[sender],
            send_sem=power_send.at[at],
            recv_sem=power_recv.at[sender],
            device_id=device,
            device_id_type=MESH,
        )

    outer_low(STEPS - 1, 0)
    outer_high(STEPS - 1, 0)
    local = jnp.zeros((TILE, depth_z), jnp.float32)
    for c in range(comps):
        for x in range(wx):
            field = elec[0, c, x, pl.ds(own, wy), :]
            square = field * field
            for k in range(wy // TILE):
                local = local + square[k * TILE : (k + 1) * TILE, :]
    local = jnp.where(lane == planes[1], jnp.sum(local, axis=0, keepdims=True), 0.0)
    power_mine[...] = local
    power_all[me] = local

    def share(j, carry):
        power_copy(j, me).start()
        return carry

    lax.fori_loop(1, group, share, 0)
    for copy in give(0):
        copy.start()

    outer_low(STEPS - 1, 1)
    outer_high(STEPS - 1, 1)
    for copy in give(1):
        copy.start()
    correlate()

    def collect(j, carry):
        at, _ = peer(j)
        power_copy(j, at).wait_recv()
        return carry

    lax.fori_loop(1, group, collect, 0)

    def add(j, total):
        return total + power_all[j]

    total = lax.fori_loop(0, group, add, jnp.zeros((1, depth_z), jnp.float32))
    power = jnp.sum(total, axis=1, keepdims=True)
    power = power / (wx * count_x * wy * count_y)
    scale = 1.0 / (power + small_eps)
    for x in range(wx):
        grad[x] = front[x] * corr[x, pl.ds(own, wy), :] * scale
    last_copy = pltpu.make_async_copy(grad, gradient_out, load_sem.at[0])
    last_copy.start()

    def sent(j, carry):
        power_copy(j, me).wait_send()
        return carry

    lax.fori_loop(1, group, sent, 0)

    def drain(e, carry):
        for s in range(sets):
            side_copy(e, s).wait_send()

            @pl.when(((gx > 0) & (gy == 0)) | ((gx < count_x - 1) & (gy == 1)))
            def _():
                slant_copy(e, s).wait_send()

            @pl.when(gx < count_x - 1)
            def _():
                up_copy(e, s).wait_send()

            @pl.when(gx > 0)
            def _():
                down_copy(e, s).wait_send()

        return carry

    lax.fori_loop(0, STEPS, drain, 0)
    for s in range(sets):
        for copy in give(s):
            copy.wait()
    last_copy.wait()


def shards(count_x, count_y, electric, magnetic, density, design_mask, planes, profiles, waveforms):
    sets, comps, wx, wy, depth_z = electric.shape
    assert count_y == 2 and wx > 1
    rows = wy
    group = count_x * count_y
    f32 = jnp.float32
    dma = pltpu.SemaphoreType.DMA
    hbm = pl.BlockSpec(memory_space=pl.ANY)
    return pl.pallas_call(
        functools.partial(kernel, count_x, count_y),
        out_shape=(
            jax.ShapeDtypeStruct(electric.shape, f32),
            jax.ShapeDtypeStruct(magnetic.shape, f32),
            jax.ShapeDtypeStruct(density.shape, f32),
        ),
        in_specs=[hbm] * 7,
        out_specs=(hbm, hbm, hbm),
        scratch_shapes=[
            pltpu.VMEM((sets, comps, wx, rows + TILE, depth_z), f32),
            pltpu.VMEM((sets, comps, wx + 1, rows + TILE, depth_z), f32),
            pltpu.VMEM((wx, rows, depth_z), f32),
            pltpu.VMEM((sets, wx, rows, depth_z), f32),
            pltpu.VMEM((wx, rows, depth_z), f32),
            pltpu.VMEM((wx, wy, depth_z), f32),
            pltpu.VMEM((STEPS, sets, 2, rows, depth_z), f32),
            pltpu.VMEM((STEPS, sets, 2, rows, depth_z), f32),
            pltpu.VMEM((STEPS, sets, 2, rows, depth_z), f32),
            pltpu.VMEM((STEPS, sets, 2, rows, depth_z), f32),
            pltpu.VMEM((STEPS, sets, 2 * wx, depth_z), f32),
            pltpu.VMEM((STEPS, sets, 2 * wx, depth_z), f32),
            pltpu.VMEM((STEPS, sets, 1, depth_z), f32),
            pltpu.VMEM((STEPS, sets, 1, depth_z), f32),
            pltpu.VMEM((1, depth_z), f32),
            pltpu.VMEM((group, 1, depth_z), f32),
            pltpu.VMEM((wx, wy, depth_z), f32),
            pltpu.VMEM(density.shape, f32),
            pltpu.VMEM(density.shape, jnp.int32),
            pltpu.SMEM(planes.shape, jnp.int32),
            pltpu.VMEM(profiles.shape, f32),
            pltpu.SMEM(waveforms.shape, f32),
            dma((7,)),
            dma((2, sets)),
            dma((STEPS, sets)),
            dma((STEPS, sets)),
            dma((STEPS, sets)),
            dma((STEPS, sets)),
            dma((STEPS, sets)),
            dma((STEPS, sets)),
            dma((STEPS, sets)),
            dma((STEPS, sets)),
            dma((group,)),
            dma((group,)),
        ],
        compiler_params=pltpu.CompilerParams(collective_id=0, has_side_effects=True),
    )(electric, magnetic, density, design_mask, planes, profiles, waveforms)


def solution(mesh):
    return jax.shard_map(
        functools.partial(shards, mesh.shape["gx"], mesh.shape["gy"]),
        mesh=mesh,
        in_specs=(
            P(None, None, ("cand", "gx"), "gy", None),
            P(None, None, ("cand", "gx"), "gy", None),
            P(("cand", "gx"), "gy", None),
            P(("cand", "gx"), "gy", None),
            P("cand"),
            P(None, ("cand", "gx"), "gy"),
            P(None, "cand"),
        ),
        out_specs=(
            P(None, None, ("cand", "gx"), "gy", None),
            P(None, None, ("cand", "gx"), "gy", None),
            P(("cand", "gx"), "gy", None),
        ),
        check_vma=False,
    )
```

```python
import functools

import jax
import jax.numpy as jnp
from jax import lax
from jax.experimental import pallas as pl
from jax.experimental.pallas import tpu as pltpu
from jax.sharding import PartitionSpec as P

STEPS = 8
PMLW = 8
TILE = 8

step_dt = 0.7
contrast = 5.0
sigma_max = 2.0
small_eps = 1e-06
inv_spacing = 0.5

MESH = pl.DeviceIdType.MESH


def coefficients(depth_cells, layer):
    zpos = lax.broadcasted_iota(jnp.int32, (1, depth_cells), 1).astype(jnp.float32)
    lower = (layer - zpos - 0.5) / layer
    upper = (zpos + 0.5 - (depth_cells - layer)) / layer
    depth = jnp.maximum(jnp.maximum(lower, upper), 0.0)
    sigma = sigma_max * depth * depth * depth
    half = sigma * step_dt / 2.0
    return ((1.0 - half) / (1.0 + half), step_dt / (1.0 + half))


def kernel(
    count_x,
    count_y,
    electric,
    magnetic,
    density_far,
    mask_far,
    planes_far,
    profiles_far,
    waves_far,
    electric_out,
    magnetic_out,
    gradient_out,
    elec,
    magn,
    scaled,
    source,
    corr,
    front,
    send_up,
    send_down,
    from_low,
    from_high,
    send_side,
    from_side,
    send_slant,
    from_slant,
    power_mine,
    power_all,
    grad,
    density,
    mask,
    planes,
    profiles,
    waves,
    load_sem,
    store_sem,
    side_sent,
    side_recv,
    slant_sent,
    slant_recv,
    up_send,
    up_recv,
    down_send,
    down_recv,
    power_send,
    power_recv,
):
    sets, comps, wx, wy, depth_z = electric.shape
    rows = wy
    edge = wy - 1
    last = wx - 1
    gx = lax.axis_index("gx")
    gy = lax.axis_index("gy")
    group = count_x * count_y
    me = gx * count_y + gy
    other = {"gy": 1 - gy}
    upper = {"gx": lax.rem(gx + 1, count_x)}
    lower = {"gx": lax.rem(gx + count_x - 1, count_x)}
    own = 0

    def peer(j):
        at = lax.rem(me + j, group)
        return at, {"gx": at // count_y, "gy": lax.rem(at, count_y)}


    small = [
        pltpu.make_async_copy(far, near, load_sem.at[2 + k])
        for k, (far, near) in enumerate(
            (
                (density_far, density),
                (mask_far, mask),
                (profiles_far, profiles),
                (planes_far, planes),
                (waves_far, waves),
            )
        )
    ]
    loads = [
        pltpu.make_async_copy(electric, elec.at[:, :, :, pl.ds(own, wy), :], load_sem.at[0]),
        pltpu.make_async_copy(
            magnetic, magn.at[:, :, pl.ds(1, wx), pl.ds(own + TILE, wy), :], load_sem.at[1]
        ),
    ]
    for load in small + loads:
        load.start()

    elec[:, :, :, rows:, :] = jnp.zeros((sets, comps, wx, TILE, depth_z), jnp.float32)
    magn[:, :, 1:, :TILE, :] = jnp.zeros((sets, comps, wx, TILE, depth_z), jnp.float32)

    barrier = pltpu.get_barrier_semaphore()

    def greet(j, carry):
        pl.semaphore_signal(barrier, inc=1, device_id=peer(j)[1], device_id_type=MESH)
        return carry

    lax.fori_loop(1, group, greet, 0)

    corr[...] = jnp.zeros_like(corr)
    decay, gain = coefficients(depth_z, PMLW)
    gain_half = gain * inv_spacing
    lane = lax.broadcasted_iota(jnp.int32, (1, depth_z), 1)
    for load in small:
        load.wait()
    flags = mask[...].astype(jnp.float32)
    inv_eps = 1.0 / (1.0 + contrast * density[...] * flags)
    front[...] = flags * contrast * inv_eps * inv_eps * step_dt
    scaled[:, pl.ds(own, wy), :] = inv_eps * gain
    eye = lax.broadcasted_iota(jnp.int32, (wy, wy), 0) == lax.broadcasted_iota(
        jnp.int32, (wy, wy), 1
    )
    for s in range(sets):
        hot = jnp.where(lane == planes[s], gain, 0.0)
        for x in range(wx):
            row = jnp.broadcast_to(profiles[s, x : x + 1, :], (wy, wy))
            column = jnp.sum(jnp.where(eye, row, 0.0), axis=1, keepdims=True)
            source[s, x, pl.ds(own, wy), :] = column * hot

    for load in loads:
        load.wait()
    pl.semaphore_wait(barrier, group - 1)

    def next_z(f):
        return jnp.where(lane < depth_z - 1, pltpu.roll(f, depth_z - 1, 1), 0.0)

    def previous_z(f):
        return jnp.where(lane > 0, pltpu.roll(f, 1, 1), 0.0)

    def side_copy(e, s):
        return pltpu.make_async_remote_copy(
            src_ref=send_side.at[e, s],
            dst_ref=from_side.at[e, s],
            send_sem=side_sent.at[e, s],
            recv_sem=side_recv.at[e, s],
            device_id=other,
            device_id_type=MESH,
        )

    def slant_copy(e, s):
        return pltpu.make_async_remote_copy(
            src_ref=send_slant.at[e, s],
            dst_ref=from_slant.at[e, s],
            send_sem=slant_sent.at[e, s],
            recv_sem=slant_recv.at[e, s],
            device_id={
                "gx": lax.rem(gx + count_x - 1 + 2 * gy, count_x),
                "gy": 1 - gy,
            },
            device_id_type=MESH,
        )

    def send_beside(e, s):
        @pl.when(gy == 0)
        def _():
            for x in range(wx):
                ex = elec[s, 0, x, edge : edge + 1, :]
                ey = elec[s, 1, x, edge : edge + 1, :]
                ez = elec[s, 2, x, edge : edge + 1, :]
                hx = magn[s, 0, x + 1, TILE + edge : TILE + wy, :]
                hz = magn[s, 2, x + 1, TILE + edge : TILE + wy, :]
                slope = ey if x == last else ey - elec[s, 1, x + 1, edge : edge + 1, :]
                send_side[e, s, x : x + 1, :] = decay * hx + gain_half * (ez + (next_z(ey) - ey))
                send_side[e, s, wx + x : wx + x + 1, :] = (
                    decay * hz + gain * slope - gain_half * ex
                )

        @pl.when(gy == 1)
        def _():
            for x in range(wx):
                send_side[e, s, x : x + 1, :] = elec[s, 0, x, 0:1, :]
                send_side[e, s, wx + x : wx + x + 1, :] = elec[s, 2, x, 0:1, :]

        side_copy(e, s).start()

    def take_beside(t, s):
        side_copy(t, s).wait_recv()

        @pl.when(gy == 0)
        def _():
            for x in range(wx):
                elec[s, 0, x, wy : wy + 1, :] = from_side[t, s, x : x + 1, :]
                elec[s, 2, x, wy : wy + 1, :] = from_side[t, s, wx + x : wx + x + 1, :]

        @pl.when(gy == 1)
        def _():
            for x in range(wx):
                magn[s, 0, x + 1, TILE - 1 : TILE, :] = (
                    from_side[t, s, x : x + 1, :] - gain_half * elec[s, 2, x, 0:1, :]
                )
                magn[s, 2, x + 1, TILE - 1 : TILE, :] = (
                    from_side[t, s, wx + x : wx + x + 1, :] + gain_half * elec[s, 0, x, 0:1, :]
                )

    below_edge = lax.broadcasted_iota(jnp.int32, (rows, depth_z), 0) < edge

    def up_copy(e, s):
        return pltpu.make_async_remote_copy(
            src_ref=send_up.at[e, s],
            dst_ref=from_low.at[e, s],
            send_sem=up_send.at[e, s],
            recv_sem=up_recv.at[e, s],
            device_id=upper,
            device_id_type=MESH,
        )

    def down_copy(e, s):
        return pltpu.make_async_remote_copy(
            src_ref=send_down.at[e, s],
            dst_ref=from_high.at[e, s],
            send_sem=down_send.at[e, s],
            recv_sem=down_recv.at[e, s],
            device_id=lower,
            device_id_type=MESH,
        )

    def send_high(e, s):
        ex = elec[s, 0, last, :rows, :]
        ey = elec[s, 1, last, :rows, :]
        ez = elec[s, 2, last, :rows, :]
        ex_y = jnp.where(below_edge, elec[s, 0, last, 1 : rows + 1, :], 0.0)
        hy = magn[s, 1, wx, TILE:, :]
        hz = magn[s, 2, wx, TILE:, :]
        send_up[e, s, 0] = decay * hy - gain_half * (next_z(ex) - ex) - gain * ez
        send_up[e, s, 1] = decay * hz + gain * ey + gain_half * (ex_y - ex)

        @pl.when((gx < count_x - 1) & (gy == 1))
        def _():
            send_slant[e, s] = elec[s, 0, last, 0:1, :]
            slant_copy(e, s).start()

        @pl.when(gx < count_x - 1)
        def _():
            up_copy(e, s).start()

    def send_low(e, s):
        send_down[e, s, 0] = elec[s, 1, 0, :rows, :]
        send_down[e, s, 1] = elec[s, 2, 0, :rows, :]

        @pl.when((gx > 0) & (gy == 0))
        def _():
            send_slant[e, s] = elec[s, 1, 0, edge : edge + 1, :]
            slant_copy(e, s).start()

        @pl.when(gx > 0)
        def _():
            down_copy(e, s).start()

    def magnetic_at(s, x, ey_next, ez_next):
        ex = elec[s, 0, x, :rows, :]
        ey = elec[s, 1, x, :rows, :]
        ez = elec[s, 2, x, :rows, :]
        ex_y = elec[s, 0, x, 1 : rows + 1, :]
        ez_y = elec[s, 2, x, 1 : rows + 1, :]
        hx = magn[s, 0, x + 1, TILE:, :]
        hy = magn[s, 1, x + 1, TILE:, :]
        hz = magn[s, 2, x + 1, TILE:, :]
        magn[s, 0, x + 1, TILE:, :] = decay * hx - gain_half * ((ez_y - ez) - (next_z(ey) - ey))
        magn[s, 1, x + 1, TILE:, :] = (
            decay * hy - gain_half * (next_z(ex) - ex) + gain * (ez_next - ez)
        )
        magn[s, 2, x + 1, TILE:, :] = (
            decay * hz - gain * (ey_next - ey) + gain_half * (ex_y - ex)
        )

    def electric_at(t, s, x):
        hx = magn[s, 0, x + 1, TILE:, :]
        hy = magn[s, 1, x + 1, TILE:, :]
        hz = magn[s, 2, x + 1, TILE:, :]
        hx_y = magn[s, 0, x + 1, TILE - 1 : TILE - 1 + rows, :]
        hz_y = magn[s, 2, x + 1, TILE - 1 : TILE - 1 + rows, :]
        hy_x = magn[s, 1, x, TILE:, :]
        hz_x = magn[s, 2, x, TILE:, :]
        weight = scaled[x]
        half = weight * inv_spacing
        elec[s, 0, x, :rows, :] = (
            decay * elec[s, 0, x, :rows, :]
            + half * ((hz - hz_y) - (hy - previous_z(hy)))
            - source[s, x] * waves[s, t]
        )
        elec[s, 1, x, :rows, :] = (
            decay * elec[s, 1, x, :rows, :]
            + half * (hx - previous_z(hx))
            - weight * (hz - hz_x)
        )
        elec[s, 2, x, :rows, :] = (
            decay * elec[s, 2, x, :rows, :] + weight * (hy - hy_x) - half * (hx - hx_y)
        )

    def inner(t, s):
        take_beside(t, s)
        for x in range(last):
            magnetic_at(s, x, elec[s, 1, x + 1, :rows, :], elec[s, 2, x + 1, :rows, :])
        for x in range(1, last):
            electric_at(t, s, x)

    def outer_high(t, s):
        @pl.when(gx < count_x - 1)
        def _():
            down_copy(t, s).wait_recv()

        keep = jnp.broadcast_to(jnp.where(gx < count_x - 1, 1, 0), (rows, depth_z)) == 1
        magnetic_at(
            s,
            last,
            jnp.where(keep, from_high[t, s, 0], 0.0),
            jnp.where(keep, from_high[t, s, 1], 0.0),
        )

        @pl.when((gx < count_x - 1) & (gy == 1))
        def _():
            slant_copy(t, s).wait_recv()
            magn[s, 2, wx, TILE - 1 : TILE, :] = (
                magn[s, 2, wx, TILE - 1 : TILE, :] - gain * from_slant[t, s]
            )

        electric_at(t, s, last)

    def outer_low(t, s):
        @pl.when(gx > 0)
        def _():
            up_copy(t, s).wait_recv()

        keep = jnp.broadcast_to(jnp.where(gx > 0, 1, 0), (rows, depth_z)) == 1
        magn[s, 1, 0, TILE:, :] = jnp.where(
            keep, from_low[t, s, 0] + gain * elec[s, 2, 0, :rows, :], 0.0
        )
        magn[s, 2, 0, TILE:, :] = jnp.where(
            keep, from_low[t, s, 1] - gain * elec[s, 1, 0, :rows, :], 0.0
        )

        @pl.when((gx > 0) & (gy == 0))
        def _():
            slant_copy(t, s).wait_recv()
            magn[s, 2, 0, TILE + edge :, :] = (
                magn[s, 2, 0, TILE + edge :, :] + gain_half * from_slant[t, s]
            )

        electric_at(t, s, 0)

    def edges(t, order, more):
        for at, (kind, s) in enumerate(order):
            if kind:
                outer_high(t, s)
                if more:
                    send_high(t + 1, s)
            else:
                outer_low(t, s)
                if more:
                    send_low(t + 1, s)
            if more and at % 2 == 1:
                send_beside(t + 1, s)

    even = lax.rem(gx, 2) == 0

    def correlate():
        for x in range(wx):
            total = corr[x]
            for c in range(comps):
                total = total + elec[0, c, x, :rows, :] * elec[1, c, x, :rows, :]
            corr[x] = total

    for s in range(sets):
        send_high(0, s)
        send_low(0, s)
        send_beside(0, s)

    for s in range(sets):
        inner(0, s)

    def step(t, carry):
        for parity in range(2):

            @pl.when(even if parity == 0 else jnp.logical_not(even))
            def _():
                near = 1 - parity
                edges(t, ((1 - near, 0), (near, 0), (1 - near, 1), (near, 1)), True)

        correlate()
        for s in range(sets):
            inner(t + 1, s)
        return carry

    lax.fori_loop(0, STEPS - 1, step, 0)

    def give(s):
        return [
            pltpu.make_async_copy(
                elec.at[s, :, :, pl.ds(own, wy), :], electric_out.at[s], store_sem.at[0, s]
            ),
            pltpu.make_async_copy(
                magn.at[s, :, pl.ds(1, wx), pl.ds(own + TILE, wy), :],
                magnetic_out.at[s],
                store_sem.at[1, s],
            ),
        ]

    def power_copy(j, sender):
        at, device = peer(j)
        return pltpu.make_async_remote_copy(
            src_ref=power_mine,
            dst_ref=power_all.at[sender],
            send_sem=power_send.at[at],
            recv_sem=power_recv.at[sender],
            device_id=device,
            device_id_type=MESH,
        )

    outer_low(STEPS - 1, 0)
    outer_high(STEPS - 1, 0)
    local = jnp.zeros((TILE, depth_z), jnp.float32)
    for c in range(comps):
        for x in range(wx):
            field = elec[0, c, x, pl.ds(own, wy), :]
            square = field * field
            for k in range(wy // TILE):
                local = local + square[k * TILE : (k + 1) * TILE, :]
    local = jnp.where(lane == planes[1], jnp.sum(local, axis=0, keepdims=True), 0.0)
    power_mine[...] = local
    power_all[me] = local

    def share(j, carry):
        power_copy(j, me).start()
        return carry

    lax.fori_loop(1, group, share, 0)
    for copy in give(0):
        copy.start()

    outer_low(STEPS - 1, 1)
    outer_high(STEPS - 1, 1)
    for copy in give(1):
        copy.start()
    correlate()

    def collect(j, carry):
        at, _ = peer(j)
        power_copy(j, at).wait_recv()
        return carry

    lax.fori_loop(1, group, collect, 0)

    def add(j, total):
        return total + power_all[j]

    total = lax.fori_loop(0, group, add, jnp.zeros((1, depth_z), jnp.float32))
    power = jnp.sum(total, axis=1, keepdims=True)
    power = power / (wx * count_x * wy * count_y)
    scale = 1.0 / (power + small_eps)
    for x in range(wx):
        grad[x] = front[x] * corr[x, pl.ds(own, wy), :] * scale
    last_copy = pltpu.make_async_copy(grad, gradient_out, load_sem.at[0])
    last_copy.start()

    def sent(j, carry):
        power_copy(j, me).wait_send()
        return carry

    lax.fori_loop(1, group, sent, 0)

    def drain(e, carry):
        for s in range(sets):
            side_copy(e, s).wait_send()

            @pl.when(((gx > 0) & (gy == 0)) | ((gx < count_x - 1) & (gy == 1)))
            def _():
                slant_copy(e, s).wait_send()

            @pl.when(gx < count_x - 1)
            def _():
                up_copy(e, s).wait_send()

            @pl.when(gx > 0)
            def _():
                down_copy(e, s).wait_send()

        return carry

    lax.fori_loop(0, STEPS, drain, 0)
    for s in range(sets):
        for copy in give(s):
            copy.wait()
    last_copy.wait()


def write_out(electric, magnetic, gradient, electric_out, magnetic_out, gradient_out, sems):
    copies = [
        pltpu.make_async_copy(near, far, sems.at[k])
        for k, (near, far) in enumerate(
            ((electric, electric_out), (magnetic, magnetic_out), (gradient, gradient_out))
        )
    ]
    for copy in copies:
        copy.start()
    for copy in copies:
        copy.wait()


def shards(count_x, count_y, electric, magnetic, density, design_mask, planes, profiles, waveforms):
    sets, comps, wx, wy, depth_z = electric.shape
    assert count_y == 2 and wx > 1
    rows = wy
    group = count_x * count_y
    f32 = jnp.float32
    dma = pltpu.SemaphoreType.DMA
    hbm = pl.BlockSpec(memory_space=pl.ANY)
    results = pl.pallas_call(
        functools.partial(kernel, count_x, count_y),
        out_shape=(
            jax.ShapeDtypeStruct(electric.shape, f32),
            jax.ShapeDtypeStruct(magnetic.shape, f32),
            jax.ShapeDtypeStruct(density.shape, f32),
        ),
        in_specs=[hbm] * 7,
        out_specs=(hbm, hbm, hbm),
        scratch_shapes=[
            pltpu.VMEM((sets, comps, wx, rows + TILE, depth_z), f32),
            pltpu.VMEM((sets, comps, wx + 1, rows + TILE, depth_z), f32),
            pltpu.VMEM((wx, rows, depth_z), f32),
            pltpu.VMEM((sets, wx, rows, depth_z), f32),
            pltpu.VMEM((wx, rows, depth_z), f32),
            pltpu.VMEM((wx, wy, depth_z), f32),
            pltpu.VMEM((STEPS, sets, 2, rows, depth_z), f32),
            pltpu.VMEM((STEPS, sets, 2, rows, depth_z), f32),
            pltpu.VMEM((STEPS, sets, 2, rows, depth_z), f32),
            pltpu.VMEM((STEPS, sets, 2, rows, depth_z), f32),
            pltpu.VMEM((STEPS, sets, 2 * wx, depth_z), f32),
            pltpu.VMEM((STEPS, sets, 2 * wx, depth_z), f32),
            pltpu.VMEM((STEPS, sets, 1, depth_z), f32),
            pltpu.VMEM((STEPS, sets, 1, depth_z), f32),
            pltpu.VMEM((1, depth_z), f32),
            pltpu.VMEM((group, 1, depth_z), f32),
            pltpu.VMEM((wx, wy, depth_z), f32),
            pltpu.VMEM(density.shape, f32),
            pltpu.VMEM(density.shape, jnp.int32),
            pltpu.SMEM(planes.shape, jnp.int32),
            pltpu.VMEM(profiles.shape, f32),
            pltpu.SMEM(waveforms.shape, f32),
            dma((7,)),
            dma((2, sets)),
            dma((STEPS, sets)),
            dma((STEPS, sets)),
            dma((STEPS, sets)),
            dma((STEPS, sets)),
            dma((STEPS, sets)),
            dma((STEPS, sets)),
            dma((STEPS, sets)),
            dma((STEPS, sets)),
            dma((group,)),
            dma((group,)),
        ],
        compiler_params=pltpu.CompilerParams(collective_id=0, has_side_effects=True),
    )(electric, magnetic, density, design_mask, planes, profiles, waveforms)
    return pl.pallas_call(
        write_out,
        out_shape=tuple(jax.ShapeDtypeStruct(r.shape, f32) for r in results),
        in_specs=[pl.BlockSpec(memory_space=pltpu.VMEM)] * 3,
        out_specs=(hbm, hbm, hbm),
        scratch_shapes=[dma((3,))],
    )(*results)


def solution(mesh):
    return jax.shard_map(
        functools.partial(shards, mesh.shape["gx"], mesh.shape["gy"]),
        mesh=mesh,
        in_specs=(
            P(None, None, ("cand", "gx"), "gy", None),
            P(None, None, ("cand", "gx"), "gy", None),
            P(("cand", "gx"), "gy", None),
            P(("cand", "gx"), "gy", None),
            P("cand"),
            P(None, ("cand", "gx"), "gy"),
            P(None, "cand"),
        ),
        out_specs=(
            P(None, None, ("cand", "gx"), "gy", None),
            P(None, None, ("cand", "gx"), "gy", None),
            P(("cand", "gx"), "gy", None),
        ),
        check_vma=False,
    )
```
